32 devices in a mesh: rows: 4 (over z), cols: 2 (over x), slabs: 4 (over y, core).
Axes of the slice: x: 2, y: 2, z: 4, core: 2. Of those that a mesh axis runs over, the one named last changes fastest.
Arguments:
- tracer: float32 [16, 128, 256, 128], P('rows', 'cols', 'slabs'), may hold values from 0.2 to 1.8
- crowding: float32 [16, 128, 256, 128], P('rows', 'cols', 'slabs'), may hold values from 0.5 to 2
Outputs:
- column_sum: float32 [16, 128, 256, 128], P('rows', 'cols', 'slabs')
- tracer_end: float32 [16, 128, 256, 128], P('rows', 'cols', 'slabs')
The draws below stay inside these ranges and needn't reach their ends.
All inputs are finite; a program needn't handle non-finite values.
Results may differ from the reference program's by a relative error of at most 0.00002.
Values sent between devices are 32-bit elements; how exact they have to be, the bound alone decides.
A program may use at most 320 MiB of HBM per device.

```python
import jax
import jax.numpy as jnp
from jax import lax

GRID_Y = 16
GRID_X = 128
GRID_Z = 256
LEVELS = 128
STEPS = 4


def shard_levels(own_key, shape, cuts, low, top_value):
    def one(dim, shards_of):
        steps = jax.random.uniform(jax.random.fold_in(jax.random.fold_in(own_key, 6), dim), (shards_of,), jnp.float32, low / len(cuts), top_value / len(cuts))
        return jnp.repeat(jnp.exp(steps), shape[dim] // shards_of).reshape((-1,) + (1,) * (len(shape) - dim - 1))

    factor_of = one(*cuts[0])
    for cut in cuts[1:]:
        factor_of = factor_of * one(*cut)
    return factor_of


def setup_inputs(seed: int = 0) -> dict:
    splits = jax.random.split(jax.random.key(seed), 3)
    tracer = jnp.clip(0.2 + 1.5999999 * jax.random.uniform(splits[0], (GRID_Y, GRID_X, GRID_Z, LEVELS), jnp.float32) ** shard_levels(splits[0], (GRID_Y, GRID_X, GRID_Z, LEVELS), ((0, 4), (1, 2), (2, 4)), -0.2, 0.2), 0.2, 1.8)
    crowding = jnp.clip(0.5 + 1.5 * jax.random.uniform(splits[1], (GRID_Y, GRID_X, GRID_Z, LEVELS), jnp.float32) ** shard_levels(splits[1], (GRID_Y, GRID_X, GRID_Z, LEVELS), ((0, 4), (1, 2), (2, 4)), -0.2, 0.2), 0.5, 2.0)
    return {"tracer": tracer, "crowding": crowding}


def inner_cells(values, dims):
    for dim in dims:
        values = lax.slice_in_dim(values, 1, values.shape[dim] - 1, axis=dim)
    return values


def side_cells(values, dim, start, dims):
    others = [other for other in dims if other != dim]
    values = inner_cells(values, others)
    return lax.slice_in_dim(values, start, start + values.shape[dim] - 2, axis=dim)


def advance(padded, crowding):
    middle = inner_cells(padded, (0, 1, 2))
    lower = [side_cells(padded, dim, 0, (0, 1, 2)) for dim in (0, 1, 2)]
    upper = [side_cells(padded, dim, 2, (0, 1, 2)) for dim in (0, 1, 2)]
    spread = lower[0] + upper[0] + lower[1] + upper[1] + lower[2] + upper[2] - 6.0 * middle
    return middle + 0.1 * spread + 0.2 * middle * (1.0 - middle * crowding)


def reference(tracer, crowding):
    for step in range(STEPS):
        tracer = advance(jnp.pad(tracer, ((1, 1), (1, 1), (1, 1), (0, 0)), mode="constant"), crowding)
    column_sum = jnp.cumsum(tracer, axis=0) / GRID_Y
    return column_sum, tracer
```

```python
import functools
import math

import jax
import jax.numpy as jnp
from jax import lax
from jax.experimental import pallas as pl
from jax.experimental.pallas import tpu as pltpu
from jax.sharding import PartitionSpec as P

STEPS = 4
CHUNK = 4
MESH = pl.DeviceIdType.MESH


def evolve(
    sizes, chunk, tracer, crowding, end, below,
    field, crowd, edge_out, edge_in, prefix_in, prefix_out,
    row_send, row_recv, col_send, col_recv, slab_send, slab_recv, pre_send, pre_recv, local_sem,
):
    depth, width, length, _ = tracer.shape
    chunks = width // chunk
    place = {axis: lax.axis_index(axis) for axis in sizes}
    has = {axis: (place[axis] > 0, place[axis] < sizes[axis] - 1) for axis in sizes}

    def other(axis, side):
        step = 1 if side else sizes[axis] - 1
        return {axis: lax.rem(place[axis] + step, sizes[axis])}

    def rows_of(c):
        return pl.ds(c * chunk, chunk), pl.ds(1 + c * chunk, chunk)

    def row_copy(step, side, c):
        slot = step % 2
        inner, padded = rows_of(c)
        if step == 0:
            source = tracer.at[depth - 1 if side else 0, inner]
        else:
            source = field.at[slot, depth if side else 1, padded]
        return pltpu.make_async_remote_copy(
            source, field.at[slot, 0 if side else depth + 1, padded],
            row_send.at[slot, side, c], row_recv.at[slot, side, c],
            device_id=other("rows", side), device_id_type=MESH,
        )

    def col_copy(step, side):
        slot = step % 2
        planes = pl.ds(1, depth)
        if step == 0:
            source = tracer.at[:, width - 1 if side else 0]
        else:
            source = field.at[slot, planes, width if side else 1]
        return pltpu.make_async_remote_copy(
            source, field.at[slot, planes, 0 if side else width + 1],
            col_send.at[slot, side], col_recv.at[slot, side],
            device_id=other("cols", side), device_id_type=MESH,
        )

    def slab_copy(step, side):
        slot = step % 2
        return pltpu.make_async_remote_copy(
            edge_out.at[slot, side], edge_in.at[slot, side],
            slab_send.at[slot, side], slab_recv.at[slot, side],
            device_id=other("slabs", side), device_id_type=MESH,
        )

    def prefix_copy(c):
        inner, _ = rows_of(c)
        return pltpu.make_async_remote_copy(
            prefix_out.at[inner], prefix_in.at[inner], pre_send.at[c], pre_recv.at[c],
            device_id=other("rows", 1), device_id_type=MESH,
        )

    load_field = pltpu.make_async_copy(tracer, field.at[0, pl.ds(1, depth), pl.ds(1, width)], local_sem.at[0])
    load_crowd = pltpu.make_async_copy(crowding, crowd, local_sem.at[1])
    load_field.start()
    load_crowd.start()

    barrier = pltpu.get_barrier_semaphore()
    greeted = 0
    for axis in sizes:
        for side in (0, 1):
            greeted += has[axis][side].astype(jnp.int32)

            @pl.when(has[axis][side])
            def _():
                pl.semaphore_signal(barrier, inc=1, device_id=other(axis, side), device_id_type=MESH)

    pl.semaphore_wait(barrier, greeted)

    def each_chunk(turn):
        lax.fori_loop(0, chunks, lambda c, carry: (turn(c), carry)[1], 0)

    def start_rows(c):
        for side in (0, 1):
            @pl.when(has["rows"][side])
            def _():
                row_copy(0, side, c).start()

    each_chunk(start_rows)
    for side in (0, 1):
        @pl.when(has["cols"][side])
        def _():
            col_copy(0, side).start()

    for side in (0, 1):
        @pl.when(jnp.logical_not(has["rows"][side]))
        def _():
            def clear(c):
                for slot in (0, 1):
                    field[slot, depth + 1 if side else 0, pl.ds(1 + c * chunk, chunk)] = jnp.zeros(
                        (chunk,) + field.shape[3:], field.dtype)
            each_chunk(clear)

        @pl.when(jnp.logical_not(has["cols"][side]))
        def _():
            for slot in (0, 1):
                for plane in range(depth):
                    field[slot, 1 + plane, width + 1 if side else 0] = jnp.zeros(field.shape[3:], field.dtype)

        @pl.when(jnp.logical_not(has["slabs"][side]))
        def _():
            for slot in (0, 1):
                edge_in[slot, 1 - side] = jnp.zeros(edge_in.shape[2:], field.dtype)

    @pl.when(jnp.logical_not(has["rows"][0]))
    def _():
        def clear(c):
            prefix_in[pl.ds(c * chunk, chunk)] = jnp.zeros((chunk,) + prefix_in.shape[1:], field.dtype)
        each_chunk(clear)

    load_field.wait()

    def pack(x, carry):
        for plane in range(depth):
            edge_out[0, 0, plane, pl.ds(x, 1), :] = field[0, 1 + plane, 1 + x, 0:1, :]
            edge_out[0, 1, plane, pl.ds(x, 1), :] = field[0, 1 + plane, 1 + x, length - 1:length, :]
        return carry

    lax.fori_loop(0, width, pack, 0)
    for side in (0, 1):
        @pl.when(has["slabs"][side])
        def _():
            slab_copy(0, side).start()

    load_crowd.wait()

    for step in range(STEPS):
        now, later = step % 2, (step + 1) % 2
        last = step == STEPS - 1
        for side in (0, 1):
            for axis, copy in (("cols", col_copy), ("slabs", slab_copy)):
                if step >= 1:
                    @pl.when(has[axis][side])
                    def _():
                        copy(step - 1, side).wait_send()

                @pl.when(has[axis][1 - side])
                def _():
                    copy(step, side).wait_recv()

        def turn(c):
            for side in (0, 1):
                if step >= 1:
                    @pl.when(has["rows"][side])
                    def _():
                        row_copy(step - 1, side, c).wait_send()

                @pl.when(has["rows"][1 - side])
                def _():
                    row_copy(step, side, c).wait_recv()

            def line(i, carry):
                x = c * chunk + i
                spot = lax.broadcasted_iota(jnp.int32, (length, field.shape[4]), 0)
                column = [field[now, plane, 1 + x] for plane in range(depth + 2)]
                total = None
                for plane in range(depth):
                    middle = column[plane + 1]
                    ahead = edge_in[now, 1, plane, pl.ds(x, 1), :]
                    behind = edge_in[now, 0, plane, pl.ds(x, 1), :]
                    lower = jnp.where(spot == 0, ahead, pltpu.roll(middle, 1, 0))
                    upper = jnp.where(spot == length - 1, behind, pltpu.roll(middle, length - 1, 0))
                    spread = (
                        column[plane] + column[plane + 2]
                        + field[now, plane + 1, x] + field[now, plane + 1, x + 2]
                        + lower + upper - 6.0 * middle
                    )
                    new = middle + 0.1 * spread + 0.2 * middle * (1.0 - middle * crowd[plane, x])
                    field[later, plane + 1, 1 + x] = new
                    if last:
                        total = new if total is None else total + new
                    else:
                        edge_out[later, 0, plane, pl.ds(x, 1), :] = new[0:1, :]
                        edge_out[later, 1, plane, pl.ds(x, 1), :] = new[length - 1:length, :]
                if last:
                    prefix_out[x] = total
                return carry

            lax.fori_loop(0, chunk, line, 0)
            if last:
                @pl.when(jnp.logical_and(jnp.logical_not(has["rows"][0]), has["rows"][1]))
                def _():
                    prefix_copy(c).start()
            else:
                for side in (0, 1):
                    @pl.when(has["rows"][side])
                    def _():
                        row_copy(step + 1, side, c).start()

        each_chunk(turn)
        if not last:
            for side in (0, 1):
                for axis, copy in (("cols", col_copy), ("slabs", slab_copy)):
                    @pl.when(has[axis][side])
                    def _():
                        copy(step + 1, side).start()

    final = STEPS % 2
    store_end = pltpu.make_async_copy(field.at[final, pl.ds(1, depth), pl.ds(1, width)], end, local_sem.at[0])
    store_end.start()

    @pl.when(has["rows"][0])
    def _():
        def forward(c):
            prefix_copy(c).wait_recv()

            @pl.when(has["rows"][1])
            def _():
                inner = pl.ds(c * chunk, chunk)
                prefix_out[inner] = prefix_out[inner] + prefix_in[inner]
                prefix_copy(c).start()
        each_chunk(forward)

    store_below = pltpu.make_async_copy(prefix_in, below, local_sem.at[1])
    store_below.start()

    def drain(c):
        for side in (0, 1):
            @pl.when(has["rows"][side])
            def _():
                row_copy(STEPS - 1, side, c).wait_send()

        @pl.when(has["rows"][1])
        def _():
            prefix_copy(c).wait_send()

    each_chunk(drain)
    for side in (0, 1):
        for axis, copy in (("cols", col_copy), ("slabs", slab_copy)):
            @pl.when(has[axis][side])
            def _():
                copy(STEPS - 1, side).wait_send()
    store_end.wait()
    store_below.wait()


def finish(count, end, below, column_sum, tracer_end):
    running = below[...]
    for plane in range(end.shape[0]):
        value = end[plane]
        running = running + value
        tracer_end[plane] = value
        column_sum[plane] = running / count


def body(sizes, tracer, crowding):
    depth, width, length, levels = tracer.shape
    kind = tracer.dtype
    chunk = math.gcd(width, CHUNK)
    chunks = width // chunk
    anywhere = pl.BlockSpec(memory_space=pl.ANY)
    dma = pltpu.SemaphoreType.DMA
    end, below = pl.pallas_call(
        functools.partial(evolve, sizes, chunk),
        out_shape=(
            jax.ShapeDtypeStruct(tracer.shape, kind),
            jax.ShapeDtypeStruct(tracer.shape[1:], kind),
        ),
        in_specs=[anywhere, anywhere],
        out_specs=(anywhere, anywhere),
        scratch_shapes=[
            pltpu.VMEM((2, depth + 2, width + 2, length, levels), kind),
            pltpu.VMEM(tracer.shape, kind),
            pltpu.VMEM((2, 2, depth, width, levels), kind),
            pltpu.VMEM((2, 2, depth, width, levels), kind),
            pltpu.VMEM(tracer.shape[1:], kind),
            pltpu.VMEM(tracer.shape[1:], kind),
            dma((2, 2, chunks)), dma((2, 2, chunks)),
            dma((2, 2)), dma((2, 2)),
            dma((2, 2)), dma((2, 2)),
            dma((chunks,)), dma((chunks,)),
            dma((2,)),
        ],
        compiler_params=pltpu.CompilerParams(
            collective_id=0, has_side_effects=True, vmem_limit_bytes=60 * 1024 * 1024
        ),
        name="evolve",
    )(tracer, crowding)

    block = math.gcd(width, 8)
    whole = pl.BlockSpec((depth, block, length, levels), lambda i: (0, i, 0, 0))
    plane = pl.BlockSpec((block, length, levels), lambda i: (i, 0, 0))
    return pl.pallas_call(
        functools.partial(finish, depth * sizes["rows"]),
        grid=(width // block,),
        out_shape=(jax.ShapeDtypeStruct(tracer.shape, kind),) * 2,
        in_specs=[whole, plane],
        out_specs=(whole, whole),
        name="finish",
    )(end, below)


def solution(mesh):
    sizes = {axis: mesh.shape[axis] for axis in ("rows", "cols", "slabs")}
    placed = P("rows", "cols", "slabs", None)
    return jax.shard_map(
        functools.partial(body, sizes),
        mesh=mesh,
        in_specs=(placed, placed),
        out_specs=(placed, placed),
        check_vma=False,
    )
```

```python
import functools
import math

import jax
import jax.numpy as jnp
from jax import lax
from jax.experimental import pallas as pl
from jax.experimental.pallas import tpu as pltpu
from jax.sharding import PartitionSpec as P

STEPS = 4
CHUNK = 4
PIECE = 1
MESH = pl.DeviceIdType.MESH


def evolve(
    sizes, chunk, piece, tracer, crowding, end, below,
    field, crowd, edge_out, edge_in, prefix_out,
    row_send, row_recv, col_send, col_recv, slab_send, slab_recv, pre_send, pre_recv, local_sem,
):
    depth, width, length, _ = tracer.shape
    chunks, pieces = width // chunk, width // piece
    place = {axis: lax.axis_index(axis) for axis in sizes}
    has = {axis: (place[axis] > 0, place[axis] < sizes[axis] - 1) for axis in sizes}

    def other(axis, side):
        step = 1 if side else sizes[axis] - 1
        return {axis: lax.rem(place[axis] + step, sizes[axis])}

    def rows_of(c):
        return pl.ds(c * chunk, chunk), pl.ds(1 + c * chunk, chunk)

    def row_copy(step, side, c):
        slot = step % 2
        inner, padded = rows_of(c)
        if step == 0:
            source = tracer.at[depth - 1 if side else 0, inner]
        else:
            source = field.at[slot, depth if side else 1, padded]
        return pltpu.make_async_remote_copy(
            source, field.at[slot, 0 if side else depth + 1, padded],
            row_send.at[slot, side, c], row_recv.at[slot, side, c],
            device_id=other("rows", side), device_id_type=MESH,
        )

    def col_copy(step, side):
        slot = step % 2
        planes = pl.ds(1, depth)
        if step == 0:
            source = tracer.at[:, width - 1 if side else 0]
        else:
            source = field.at[slot, planes, width if side else 1]
        return pltpu.make_async_remote_copy(
            source, field.at[slot, planes, 0 if side else width + 1],
            col_send.at[slot, side], col_recv.at[slot, side],
            device_id=other("cols", side), device_id_type=MESH,
        )

    def slab_copy(step, side):
        slot = step % 2
        return pltpu.make_async_remote_copy(
            edge_out.at[slot, side], edge_in.at[slot, side],
            slab_send.at[slot, side], slab_recv.at[slot, side],
            device_id=other("slabs", side), device_id_type=MESH,
        )

    def prefix_copy(c):
        inner = pl.ds(c * piece, piece)
        return pltpu.make_async_remote_copy(
            prefix_out.at[inner], below.at[inner], pre_send.at[c], pre_recv.at[c],
            device_id=other("rows", 1), device_id_type=MESH,
        )

    load_field = pltpu.make_async_copy(tracer, field.at[0, pl.ds(1, depth), pl.ds(1, width)], local_sem.at[0])
    load_crowd = pltpu.make_async_copy(crowding, crowd, local_sem.at[1])
    load_field.start()
    load_crowd.start()

    barrier = pltpu.get_barrier_semaphore()
    greeted = 0
    for axis in sizes:
        for side in (0, 1):
            greeted += has[axis][side].astype(jnp.int32)

            @pl.when(has[axis][side])
            def _():
                pl.semaphore_signal(barrier, inc=1, device_id=other(axis, side), device_id_type=MESH)

    pl.semaphore_wait(barrier, greeted)

    def each(count, turn):
        lax.fori_loop(0, count, lambda c, carry: (turn(c), carry)[1], 0)

    def start_rows(c):
        for side in (0, 1):
            @pl.when(has["rows"][side])
            def _():
                row_copy(0, side, c).start()

    each(chunks, start_rows)
    for side in (0, 1):
        @pl.when(has["cols"][side])
        def _():
            col_copy(0, side).start()

    for side in (0, 1):
        @pl.when(jnp.logical_not(has["rows"][side]))
        def _():
            def clear(c):
                for slot in (0, 1):
                    field[slot, depth + 1 if side else 0, pl.ds(1 + c * chunk, chunk)] = jnp.zeros(
                        (chunk,) + field.shape[3:], field.dtype)
            each(chunks, clear)

        @pl.when(jnp.logical_not(has["cols"][side]))
        def _():
            for slot in (0, 1):
                for plane in range(depth):
                    field[slot, 1 + plane, width + 1 if side else 0] = jnp.zeros(field.shape[3:], field.dtype)

        @pl.when(jnp.logical_not(has["slabs"][side]))
        def _():
            for slot in (0, 1):
                edge_in[slot, 1 - side] = jnp.zeros(edge_in.shape[2:], field.dtype)

    @pl.when(jnp.logical_not(has["rows"][0]))
    def _():
        def clear(c):
            below[pl.ds(c * chunk, chunk)] = jnp.zeros((chunk,) + below.shape[1:], field.dtype)
        each(chunks, clear)

    load_field.wait()

    def pack(x, carry):
        for plane in range(depth):
            edge_out[0, 0, plane, pl.ds(x, 1), :] = field[0, 1 + plane, 1 + x, 0:1, :]
            edge_out[0, 1, plane, pl.ds(x, 1), :] = field[0, 1 + plane, 1 + x, length - 1:length, :]
        return carry

    lax.fori_loop(0, width, pack, 0)
    for side in (0, 1):
        @pl.when(has["slabs"][side])
        def _():
            slab_copy(0, side).start()

    load_crowd.wait()

    for step in range(STEPS):
        now, later = step % 2, (step + 1) % 2
        last = step == STEPS - 1
        for side in (0, 1):
            for axis, copy in (("cols", col_copy), ("slabs", slab_copy)):
                if step >= 1:
                    @pl.when(has[axis][side])
                    def _():
                        copy(step - 1, side).wait_send()

                @pl.when(has[axis][1 - side])
                def _():
                    copy(step, side).wait_recv()

        def turn(c):
            for side in (0, 1):
                if step >= 1:
                    @pl.when(has["rows"][side])
                    def _():
                        row_copy(step - 1, side, c).wait_send()

                @pl.when(has["rows"][1 - side])
                def _():
                    row_copy(step, side, c).wait_recv()

            def line(i, carry):
                x = c * chunk + i
                spot = lax.broadcasted_iota(jnp.int32, (length, field.shape[4]), 0)
                column = [field[now, plane, 1 + x] for plane in range(depth + 2)]
                total = None
                for plane in range(depth):
                    middle = column[plane + 1]
                    ahead = edge_in[now, 1, plane, pl.ds(x, 1), :]
                    behind = edge_in[now, 0, plane, pl.ds(x, 1), :]
                    lower = jnp.where(spot == 0, ahead, pltpu.roll(middle, 1, 0))
                    upper = jnp.where(spot == length - 1, behind, pltpu.roll(middle, length - 1, 0))
                    spread = (
                        column[plane] + column[plane + 2]
                        + field[now, plane + 1, x] + field[now, plane + 1, x + 2]
                        + lower + upper - 6.0 * middle
                    )
                    new = middle + 0.1 * spread + 0.2 * middle * (1.0 - middle * crowd[plane, x])
                    if last:
                        end[plane, x] = new
                        total = new if total is None else total + new
                    else:
                        field[later, plane + 1, 1 + x] = new
                        edge_out[later, 0, plane, pl.ds(x, 1), :] = new[0:1, :]
                        edge_out[later, 1, plane, pl.ds(x, 1), :] = new[length - 1:length, :]
                if last:
                    prefix_out[x] = total
                return carry

            lax.fori_loop(0, chunk, line, 0)
            if last:
                @pl.when(jnp.logical_and(jnp.logical_not(has["rows"][0]), has["rows"][1]))
                def _():
                    for k in range(chunk // piece):
                        prefix_copy(c * (chunk // piece) + k).start()
            else:
                for side in (0, 1):
                    @pl.when(has["rows"][side])
                    def _():
                        row_copy(step + 1, side, c).start()

        each(chunks, turn)
        if not last:
            for side in (0, 1):
                for axis, copy in (("cols", col_copy), ("slabs", slab_copy)):
                    @pl.when(has[axis][side])
                    def _():
                        copy(step + 1, side).start()

    @pl.when(has["rows"][0])
    def _():
        def forward(c):
            prefix_copy(c).wait_recv()

            @pl.when(has["rows"][1])
            def _():
                inner = pl.ds(c * piece, piece)
                prefix_out[inner] = prefix_out[inner] + below[inner]
                prefix_copy(c).start()
        each(pieces, forward)

    def drain(c):
        for side in (0, 1):
            @pl.when(has["rows"][side])
            def _():
                row_copy(STEPS - 1, side, c).wait_send()

    each(chunks, drain)

    @pl.when(has["rows"][1])
    def _():
        each(pieces, lambda c: prefix_copy(c).wait_send())

    for side in (0, 1):
        for axis, copy in (("cols", col_copy), ("slabs", slab_copy)):
            @pl.when(has[axis][side])
            def _():
                copy(STEPS - 1, side).wait_send()


def finish(count, block, end, below, column_sum, tracer_end, running_sum, sems):
    depth, width = end.shape[:2]
    blocks = width // block
    store_end = pltpu.make_async_copy(end, tracer_end, sems.at[blocks])
    store_end.start()

    def store_sum(b):
        lines = pl.ds(b * block, block)
        return pltpu.make_async_copy(running_sum.at[:, lines], column_sum.at[:, lines], sems.at[b])

    def turn(b, carry):
        def line(i, carry):
            x = b * block + i
            running = below[x]
            for plane in range(depth):
                running = running + end[plane, x]
                running_sum[plane, x] = running / count
            return carry

        lax.fori_loop(0, block, line, 0)
        store_sum(b).start()
        return carry

    lax.fori_loop(0, blocks, turn, 0)
    store_end.wait()
    lax.fori_loop(0, blocks, lambda b, carry: (store_sum(b).wait(), carry)[1], 0)


def body(sizes, tracer, crowding):
    depth, width, length, levels = tracer.shape
    kind = tracer.dtype
    chunk = math.gcd(width, CHUNK)
    piece = math.gcd(chunk, PIECE)
    chunks, pieces = width // chunk, width // piece
    anywhere = pl.BlockSpec(memory_space=pl.ANY)
    held = pl.BlockSpec(memory_space=pltpu.VMEM)
    dma = pltpu.SemaphoreType.DMA
    end, below = pl.pallas_call(
        functools.partial(evolve, sizes, chunk, piece),
        out_shape=(
            pltpu.VMEM(tracer.shape, kind),
            pltpu.VMEM(tracer.shape[1:], kind),
        ),
        in_specs=[anywhere, anywhere],
        out_specs=(held, held),
        scratch_shapes=[
            pltpu.VMEM((2, depth + 2, width + 2, length, levels), kind),
            pltpu.VMEM(tracer.shape, kind),
            pltpu.VMEM((2, 2, depth, width, levels), kind),
            pltpu.VMEM((2, 2, depth, width, levels), kind),
            pltpu.VMEM(tracer.shape[1:], kind),
            dma((2, 2, chunks)), dma((2, 2, chunks)),
            dma((2, 2)), dma((2, 2)),
            dma((2, 2)), dma((2, 2)),
            dma((pieces,)), dma((pieces,)),
            dma((2,)),
        ],
        compiler_params=pltpu.CompilerParams(
            collective_id=0, has_side_effects=True, vmem_limit_bytes=50 * 1024 * 1024
        ),
        name="evolve",
    )(tracer, crowding)

    block = math.gcd(width, 8)
    return pl.pallas_call(
        functools.partial(finish, depth * sizes["rows"], block),
        out_shape=(jax.ShapeDtypeStruct(tracer.shape, kind),) * 2,
        in_specs=[held, held],
        out_specs=(pl.BlockSpec(memory_space=pltpu.HBM),) * 2,
        scratch_shapes=[pltpu.VMEM(tracer.shape, kind), dma((width // block + 1,))],
        compiler_params=pltpu.CompilerParams(vmem_limit_bytes=16 * 1024 * 1024),
        name="finish",
    )(end, below)


def solution(mesh):
    sizes = {axis: mesh.shape[axis] for axis in ("rows", "cols", "slabs")}
    placed = P("rows", "cols", "slabs", None)
    return jax.shard_map(
        functools.partial(body, sizes),
        mesh=mesh,
        in_specs=(placed, placed),
        out_specs=(placed, placed),
        check_vma=False,
    )
```

```python
import functools
import math

import jax
import jax.numpy as jnp
from jax import lax
from jax.experimental import pallas as pl
from jax.experimental.pallas import tpu as pltpu
from jax.sharding import PartitionSpec as P

STEPS = 4
CHUNK = 4
PARTS = 2
MESH = pl.DeviceIdType.MESH


def evolve(
    sizes, chunk, parts, tracer, crowding, end, column_sum,
    field, crowd, edge_out, edge_in, below, prefix_out,
    row_send, row_recv, col_send, col_recv, slab_send, slab_recv, pre_send, pre_recv, local_sem,
):
    depth, width, length, _ = tracer.shape
    chunks, pieces = width // chunk, width * parts
    place = {axis: lax.axis_index(axis) for axis in sizes}
    has = {axis: (place[axis] > 0, place[axis] < sizes[axis] - 1) for axis in sizes}

    def other(axis, side):
        step = 1 if side else sizes[axis] - 1
        return {axis: lax.rem(place[axis] + step, sizes[axis])}

    def rows_of(c):
        return pl.ds(c * chunk, chunk), pl.ds(1 + c * chunk, chunk)

    def row_copy(step, side, c):
        slot = step % 2
        inner, padded = rows_of(c)
        if step == 0:
            source = tracer.at[depth - 1 if side else 0, inner]
        else:
            source = field.at[slot, depth if side else 1, padded]
        return pltpu.make_async_remote_copy(
            source, field.at[slot, 0 if side else depth + 1, padded],
            row_send.at[slot, side, c], row_recv.at[slot, side, c],
            device_id=other("rows", side), device_id_type=MESH,
        )

    def col_copy(step, side):
        slot = step % 2
        planes = pl.ds(1, depth)
        if step == 0:
            source = tracer.at[:, width - 1 if side else 0]
        else:
            source = field.at[slot, planes, width if side else 1]
        return pltpu.make_async_remote_copy(
            source, field.at[slot, planes, 0 if side else width + 1],
            col_send.at[slot, side], col_recv.at[slot, side],
            device_id=other("cols", side), device_id_type=MESH,
        )

    def slab_copy(step, side):
        slot = step % 2
        return pltpu.make_async_remote_copy(
            edge_out.at[slot, side], edge_in.at[slot, side],
            slab_send.at[slot, side], slab_recv.at[slot, side],
            device_id=other("slabs", side), device_id_type=MESH,
        )

    def piece_of(c):
        part = length // parts
        return c // parts, pl.ds(pl.multiple_of((c % parts) * part, part), part)

    def prefix_copy(c):
        inner = piece_of(c)
        return pltpu.make_async_remote_copy(
            prefix_out.at[inner], below.at[inner], pre_send.at[c], pre_recv.at[c],
            device_id=other("rows", 1), device_id_type=MESH,
        )

    load_field = pltpu.make_async_copy(tracer, field.at[0, pl.ds(1, depth), pl.ds(1, width)], local_sem.at[0])
    load_crowd = pltpu.make_async_copy(crowding, crowd, local_sem.at[1])
    load_field.start()

    barrier = pltpu.get_barrier_semaphore()
    greeted = 0
    for axis in sizes:
        for side in (0, 1):
            greeted += has[axis][side].astype(jnp.int32)

            @pl.when(has[axis][side])
            def _():
                pl.semaphore_signal(barrier, inc=1, device_id=other(axis, side), device_id_type=MESH)

    pl.semaphore_wait(barrier, greeted)

    def each(count, turn):
        lax.fori_loop(0, count, lambda c, carry: (turn(c), carry)[1], 0)

    def start_rows(c):
        for side in (0, 1):
            @pl.when(has["rows"][side])
            def _():
                row_copy(0, side, c).start()

    each(chunks, start_rows)
    load_crowd.start()
    for side in (0, 1):
        @pl.when(has["cols"][side])
        def _():
            col_copy(0, side).start()

    for side in (0, 1):
        @pl.when(jnp.logical_not(has["rows"][side]))
        def _():
            def clear(c):
                for slot in (0, 1):
                    field[slot, depth + 1 if side else 0, pl.ds(1 + c * chunk, chunk)] = jnp.zeros(
                        (chunk,) + field.shape[3:], field.dtype)
            each(chunks, clear)

        @pl.when(jnp.logical_not(has["cols"][side]))
        def _():
            for slot in (0, 1):
                for plane in range(depth):
                    field[slot, 1 + plane, width + 1 if side else 0] = jnp.zeros(field.shape[3:], field.dtype)

        @pl.when(jnp.logical_not(has["slabs"][side]))
        def _():
            for slot in (0, 1):
                edge_in[slot, 1 - side] = jnp.zeros(edge_in.shape[2:], field.dtype)

    @pl.when(jnp.logical_not(has["rows"][0]))
    def _():
        def clear(c):
            below[pl.ds(c * chunk, chunk)] = jnp.zeros((chunk,) + below.shape[1:], field.dtype)
        each(chunks, clear)

    load_field.wait()

    def pack(x, carry):
        for plane in range(depth):
            edge_out[0, 0, plane, pl.ds(x, 1), :] = field[0, 1 + plane, 1 + x, 0:1, :]
            edge_out[0, 1, plane, pl.ds(x, 1), :] = field[0, 1 + plane, 1 + x, length - 1:length, :]
        return carry

    lax.fori_loop(0, width, pack, 0)
    for side in (0, 1):
        @pl.when(has["slabs"][side])
        def _():
            slab_copy(0, side).start()

    load_crowd.wait()

    for step in range(STEPS):
        now, later = step % 2, (step + 1) % 2
        last = step == STEPS - 1
        for side in (0, 1):
            for axis, copy in (("cols", col_copy), ("slabs", slab_copy)):
                if step >= 1:
                    @pl.when(has[axis][side])
                    def _():
                        copy(step - 1, side).wait_send()

                @pl.when(has[axis][1 - side])
                def _():
                    copy(step, side).wait_recv()

        def turn(c):
            for side in (0, 1):
                if step >= 1:
                    @pl.when(has["rows"][side])
                    def _():
                        row_copy(step - 1, side, c).wait_send()

                @pl.when(has["rows"][1 - side])
                def _():
                    row_copy(step, side, c).wait_recv()

            def line(i, carry):
                x = c * chunk + i
                spot = lax.broadcasted_iota(jnp.int32, (length, field.shape[4]), 0)
                column = [field[now, plane, 1 + x] for plane in range(depth + 2)]
                total = None
                for plane in range(depth):
                    middle = column[plane + 1]
                    ahead = edge_in[now, 1, plane, pl.ds(x, 1), :]
                    behind = edge_in[now, 0, plane, pl.ds(x, 1), :]
                    lower = jnp.where(spot == 0, ahead, pltpu.roll(middle, 1, 0))
                    upper = jnp.where(spot == length - 1, behind, pltpu.roll(middle, length - 1, 0))
                    spread = (
                        column[plane] + column[plane + 2]
                        + field[now, plane + 1, x] + field[now, plane + 1, x + 2]
                        + lower + upper - 6.0 * middle
                    )
                    new = middle + 0.1 * spread + 0.2 * middle * (1.0 - middle * crowd[plane, x])
                    if last:
                        end[plane, x] = new
                        total = new if total is None else total + new
                    else:
                        field[later, plane + 1, 1 + x] = new
                        edge_out[later, 0, plane, pl.ds(x, 1), :] = new[0:1, :]
                        edge_out[later, 1, plane, pl.ds(x, 1), :] = new[length - 1:length, :]
                if last:
                    prefix_out[x] = total
                return carry

            lax.fori_loop(0, chunk, line, 0)
            if last:
                @pl.when(jnp.logical_and(jnp.logical_not(has["rows"][0]), has["rows"][1]))
                def _():
                    for k in range(chunk * parts):
                        prefix_copy(c * (chunk * parts) + k).start()
            else:
                for side in (0, 1):
                    @pl.when(has["rows"][side])
                    def _():
                        row_copy(step + 1, side, c).start()

        each(chunks, turn)
        if not last:
            for side in (0, 1):
                for axis, copy in (("cols", col_copy), ("slabs", slab_copy)):
                    @pl.when(has[axis][side])
                    def _():
                        copy(step + 1, side).start()

    def drain(side):
        @pl.when(has["rows"][side])
        def _():
            each(chunks, lambda c: row_copy(STEPS - 1, side, c).wait_send())

    drain(0)
    for side in (0, 1):
        for axis, copy in (("cols", col_copy), ("slabs", slab_copy)):
            @pl.when(has[axis][side])
            def _():
                copy(STEPS - 1, side).wait_send()

    share = 1.0 / (depth * sizes["rows"])

    def forward(c):
        x, part = piece_of(c)

        @pl.when(has["rows"][0])
        def _():
            prefix_copy(c).wait_recv()

            @pl.when(has["rows"][1])
            def _():
                prefix_out[x, part] = prefix_out[x, part] + below[x, part]
                prefix_copy(c).start()

        running = below[x, part]
        for plane in range(depth):
            running = running + end[plane, x, part]
            column_sum[plane, x, part] = running * share

    each(pieces, forward)
    drain(1)

    @pl.when(has["rows"][1])
    def _():
        each(pieces, lambda c: prefix_copy(c).wait_send())


def finish(*refs):
    held, placed, sems = refs[:2], refs[2:4], refs[4]
    depth = held[0].shape[0]
    copies = [
        pltpu.make_async_copy(held[k].at[plane], placed[k].at[plane], sems.at[k, plane])
        for k in range(2) for plane in range(depth)
    ]
    for copy in copies:
        copy.start()
    for copy in copies:
        copy.wait()


def body(sizes, tracer, crowding):
    depth, width, length, levels = tracer.shape
    kind = tracer.dtype
    chunk = math.gcd(width, CHUNK)
    parts = PARTS if length % (8 * PARTS) == 0 else 1
    chunks, pieces = width // chunk, width * parts
    anywhere = pl.BlockSpec(memory_space=pl.ANY)
    held = pl.BlockSpec(memory_space=pltpu.VMEM)
    dma = pltpu.SemaphoreType.DMA
    end, column_sum = pl.pallas_call(
        functools.partial(evolve, sizes, chunk, parts),
        out_shape=(
            pltpu.VMEM(tracer.shape, kind),
            pltpu.VMEM(tracer.shape, kind),
        ),
        in_specs=[anywhere, anywhere],
        out_specs=(held, held),
        scratch_shapes=[
            pltpu.VMEM((2, depth + 2, width + 2, length, levels), kind),
            pltpu.VMEM(tracer.shape, kind),
            pltpu.VMEM((2, 2, depth, width, levels), kind),
            pltpu.VMEM((2, 2, depth, width, levels), kind),
            pltpu.VMEM(tracer.shape[1:], kind),
            pltpu.VMEM(tracer.shape[1:], kind),
            dma((2, 2, chunks)), dma((2, 2, chunks)),
            dma((2, 2)), dma((2, 2)),
            dma((2, 2)), dma((2, 2)),
            dma((pieces,)), dma((pieces,)),
            dma((2,)),
        ],
        compiler_params=pltpu.CompilerParams(
            collective_id=0, has_side_effects=True, vmem_limit_bytes=42 * 1024 * 1024
        ),
        name="evolve",
    )(tracer, crowding)

    return pl.pallas_call(
        finish,
        out_shape=(jax.ShapeDtypeStruct(tracer.shape, kind),) * 2,
        in_specs=[held, held],
        out_specs=(pl.BlockSpec(memory_space=pltpu.HBM),) * 2,
        scratch_shapes=[dma((2, depth))],
        compiler_params=pltpu.CompilerParams(vmem_limit_bytes=1024 * 1024),
        name="finish",
    )(column_sum, end)


def solution(mesh):
    sizes = {axis: mesh.shape[axis] for axis in ("rows", "cols", "slabs")}
    placed = P("rows", "cols", "slabs", None)
    return jax.shard_map(
        functools.partial(body, sizes),
        mesh=mesh,
        in_specs=(placed, placed),
        out_specs=(placed, placed),
        check_vma=False,
    )
```

```python
import functools
import math

import jax
import jax.numpy as jnp
from jax import lax
from jax.experimental import pallas as pl
from jax.experimental.pallas import tpu as pltpu
from jax.sharding import PartitionSpec as P

STEPS = 4
CHUNK = 8
PARTS = 1
MESH = pl.DeviceIdType.MESH


def evolve(
    sizes, chunk, parts, tracer, crowding, end, column_sum,
    field, crowd, edge_out, edge_in, below, prefix_out,
    row_send, row_recv, col_send, col_recv, slab_send, slab_recv, pre_send, pre_recv, local_sem,
):
    depth, width, length, _ = tracer.shape
    chunks, pieces = width // chunk, width * parts
    place = {axis: lax.axis_index(axis) for axis in sizes}
    has = {axis: (place[axis] > 0, place[axis] < sizes[axis] - 1) for axis in sizes}

    def other(axis, side):
        step = 1 if side else sizes[axis] - 1
        return {axis: lax.rem(place[axis] + step, sizes[axis])}

    def rows_of(c):
        return pl.ds(c * chunk, chunk), pl.ds(1 + c * chunk, chunk)

    def row_copy(step, side, c):
        slot = step % 2
        inner, padded = rows_of(c)
        if step == 0:
            source = tracer.at[depth - 1 if side else 0, inner]
        else:
            source = field.at[slot, depth if side else 1, padded]
        return pltpu.make_async_remote_copy(
            source, field.at[slot, 0 if side else depth + 1, padded],
            row_send.at[slot, side, c], row_recv.at[slot, side, c],
            device_id=other("rows", side), device_id_type=MESH,
        )

    def col_copy(step, side):
        slot = step % 2
        planes = pl.ds(1, depth)
        if step == 0:
            source = tracer.at[:, width - 1 if side else 0]
        else:
            source = field.at[slot, planes, width if side else 1]
        return pltpu.make_async_remote_copy(
            source, field.at[slot, planes, 0 if side else width + 1],
            col_send.at[slot, side], col_recv.at[slot, side],
            device_id=other("cols", side), device_id_type=MESH,
        )

    def slab_copy(step, side):
        slot = step % 2
        return pltpu.make_async_remote_copy(
            edge_out.at[slot, side], edge_in.at[slot, side],
            slab_send.at[slot, side], slab_recv.at[slot, side],
            device_id=other("slabs", side), device_id_type=MESH,
        )

    def piece_of(c):
        part = length // parts
        return c // parts, pl.ds(pl.multiple_of((c % parts) * part, part), part)

    def prefix_copy(c):
        inner = piece_of(c)
        return pltpu.make_async_remote_copy(
            prefix_out.at[inner], below.at[inner], pre_send.at[c], pre_recv.at[c],
            device_id=other("rows", 1), device_id_type=MESH,
        )

    load_field = pltpu.make_async_copy(tracer, field.at[0, pl.ds(1, depth), pl.ds(1, width)], local_sem.at[0])
    load_crowd = pltpu.make_async_copy(crowding, crowd, local_sem.at[1])
    load_field.start()

    barrier = pltpu.get_barrier_semaphore()
    greeted = 0
    for axis in sizes:
        for side in (0, 1):
            greeted += has[axis][side].astype(jnp.int32)

            @pl.when(has[axis][side])
            def _():
                pl.semaphore_signal(barrier, inc=1, device_id=other(axis, side), device_id_type=MESH)

    pl.semaphore_wait(barrier, greeted)

    def each(count, turn):
        lax.fori_loop(0, count, lambda c, carry: (turn(c), carry)[1], 0)

    def start_rows(c):
        for side in (0, 1):
            @pl.when(has["rows"][side])
            def _():
                row_copy(0, side, c).start()

    each(chunks, start_rows)
    load_crowd.start()
    for side in (0, 1):
        @pl.when(has["cols"][side])
        def _():
            col_copy(0, side).start()

    for side in (0, 1):
        @pl.when(jnp.logical_not(has["rows"][side]))
        def _():
            def clear(c):
                for slot in (0, 1):
                    field[slot, depth + 1 if side else 0, pl.ds(1 + c * chunk, chunk)] = jnp.zeros(
                        (chunk,) + field.shape[3:], field.dtype)
            each(chunks, clear)

        @pl.when(jnp.logical_not(has["cols"][side]))
        def _():
            for slot in (0, 1):
                for plane in range(depth):
                    field[slot, 1 + plane, width + 1 if side else 0] = jnp.zeros(field.shape[3:], field.dtype)

        @pl.when(jnp.logical_not(has["slabs"][side]))
        def _():
            for slot in (0, 1):
                edge_in[slot, 1 - side] = jnp.zeros(edge_in.shape[2:], field.dtype)

    @pl.when(jnp.logical_not(has["rows"][0]))
    def _():
        def clear(c):
            below[pl.ds(c * chunk, chunk)] = jnp.zeros((chunk,) + below.shape[1:], field.dtype)
        each(chunks, clear)

    load_field.wait()

    def pack(x, carry):
        for plane in range(depth):
            edge_out[0, 0, plane, pl.ds(x, 1), :] = field[0, 1 + plane, 1 + x, 0:1, :]
            edge_out[0, 1, plane, pl.ds(x, 1), :] = field[0, 1 + plane, 1 + x, length - 1:length, :]
        return carry

    lax.fori_loop(0, width, pack, 0)
    for side in (0, 1):
        @pl.when(has["slabs"][side])
        def _():
            slab_copy(0, side).start()

    load_crowd.wait()

    for step in range(STEPS):
        now, later = step % 2, (step + 1) % 2
        last = step == STEPS - 1
        for side in (0, 1):
            for axis, copy in (("cols", col_copy), ("slabs", slab_copy)):
                if step >= 1:
                    @pl.when(has[axis][side])
                    def _():
                        copy(step - 1, side).wait_send()

                @pl.when(has[axis][1 - side])
                def _():
                    copy(step, side).wait_recv()

        def turn(c):
            for side in (0, 1):
                if step >= 1:
                    @pl.when(has["rows"][side])
                    def _():
                        row_copy(step - 1, side, c).wait_send()

                @pl.when(has["rows"][1 - side])
                def _():
                    row_copy(step, side, c).wait_recv()

            def line(i, carry):
                x = c * chunk + i
                spot = lax.broadcasted_iota(jnp.int32, (length, field.shape[4]), 0)
                column = [field[now, plane, 1 + x] for plane in range(depth + 2)]
                total = None
                for plane in range(depth):
                    middle = column[plane + 1]
                    ahead = edge_in[now, 1, plane, pl.ds(x, 1), :]
                    behind = edge_in[now, 0, plane, pl.ds(x, 1), :]
                    lower = jnp.where(spot == 0, ahead, pltpu.roll(middle, 1, 0))
                    upper = jnp.where(spot == length - 1, behind, pltpu.roll(middle, length - 1, 0))
                    spread = (
                        column[plane] + column[plane + 2]
                        + field[now, plane + 1, x] + field[now, plane + 1, x + 2]
                        + lower + upper - 6.0 * middle
                    )
                    new = middle + 0.1 * spread + 0.2 * middle * (1.0 - middle * crowd[plane, x])
                    if last:
                        end[plane, x] = new
                        total = new if total is None else total + new
                    else:
                        field[later, plane + 1, 1 + x] = new
                        edge_out[later, 0, plane, pl.ds(x, 1), :] = new[0:1, :]
                        edge_out[later, 1, plane, pl.ds(x, 1), :] = new[length - 1:length, :]
                if last:
                    prefix_out[x] = total
                return carry

            lax.fori_loop(0, chunk, line, 0)
            if last:
                @pl.when(jnp.logical_and(jnp.logical_not(has["rows"][0]), has["rows"][1]))
                def _():
                    for k in range(chunk * parts):
                        prefix_copy(c * (chunk * parts) + k).start()
            else:
                for side in (0, 1):
                    @pl.when(has["rows"][side])
                    def _():
                        row_copy(step + 1, side, c).start()

        each(chunks, turn)
        if not last:
            for side in (0, 1):
                for axis, copy in (("cols", col_copy), ("slabs", slab_copy)):
                    @pl.when(has[axis][side])
                    def _():
                        copy(step + 1, side).start()

    def drain(side):
        @pl.when(has["rows"][side])
        def _():
            each(chunks, lambda c: row_copy(STEPS - 1, side, c).wait_send())

    drain(0)
    for side in (0, 1):
        for axis, copy in (("cols", col_copy), ("slabs", slab_copy)):
            @pl.when(has[axis][side])
            def _():
                copy(STEPS - 1, side).wait_send()

    share = 1.0 / (depth * sizes["rows"])

    def forward(c):
        x, part = piece_of(c)

        @pl.when(has["rows"][0])
        def _():
            prefix_copy(c).wait_recv()

            @pl.when(has["rows"][1])
            def _():
                prefix_out[x, part] = prefix_out[x, part] + below[x, part]
                prefix_copy(c).start()

        running = below[x, part]
        for plane in range(depth):
            running = running + end[plane, x, part]
            column_sum[plane, x, part] = running * share

    each(pieces, forward)
    drain(1)

    @pl.when(has["rows"][1])
    def _():
        each(pieces, lambda c: prefix_copy(c).wait_send())


def finish(*refs):
    held, placed, sems = refs[:2], refs[2:4], refs[4]
    depth = held[0].shape[0]
    copies = [
        pltpu.make_async_copy(held[k].at[plane], placed[k].at[plane], sems.at[k, plane])
        for k in range(2) for plane in range(depth)
    ]
    for copy in copies:
        copy.start()
    for copy in copies:
        copy.wait()


def body(sizes, tracer, crowding):
    depth, width, length, levels = tracer.shape
    kind = tracer.dtype
    chunk = math.gcd(width, CHUNK)
    parts = PARTS if length % (8 * PARTS) == 0 else 1
    chunks, pieces = width // chunk, width * parts
    anywhere = pl.BlockSpec(memory_space=pl.ANY)
    held = pl.BlockSpec(memory_space=pltpu.VMEM)
    dma = pltpu.SemaphoreType.DMA
    end, column_sum = pl.pallas_call(
        functools.partial(evolve, sizes, chunk, parts),
        out_shape=(
            pltpu.VMEM(tracer.shape, kind),
            pltpu.VMEM(tracer.shape, kind),
        ),
        in_specs=[anywhere, anywhere],
        out_specs=(held, held),
        scratch_shapes=[
            pltpu.VMEM((2, depth + 2, width + 2, length, levels), kind),
            pltpu.VMEM(tracer.shape, kind),
            pltpu.VMEM((2, 2, depth, width, levels), kind),
            pltpu.VMEM((2, 2, depth, width, levels), kind),
            pltpu.VMEM(tracer.shape[1:], kind),
            pltpu.VMEM(tracer.shape[1:], kind),
            dma((2, 2, chunks)), dma((2, 2, chunks)),
            dma((2, 2)), dma((2, 2)),
            dma((2, 2)), dma((2, 2)),
            dma((pieces,)), dma((pieces,)),
            dma((2,)),
        ],
        compiler_params=pltpu.CompilerParams(
            collective_id=0, has_side_effects=True, vmem_limit_bytes=42 * 1024 * 1024
        ),
        name="evolve",
    )(tracer, crowding)

    return pl.pallas_call(
        finish,
        out_shape=(jax.ShapeDtypeStruct(tracer.shape, kind),) * 2,
        in_specs=[held, held],
        out_specs=(pl.BlockSpec(memory_space=pltpu.HBM),) * 2,
        scratch_shapes=[dma((2, depth))],
        compiler_params=pltpu.CompilerParams(vmem_limit_bytes=1024 * 1024),
        name="finish",
    )(column_sum, end)


def solution(mesh):
    sizes = {axis: mesh.shape[axis] for axis in ("rows", "cols", "slabs")}
    placed = P("rows", "cols", "slabs", None)
    return jax.shard_map(
        functools.partial(body, sizes),
        mesh=mesh,
        in_specs=(placed, placed),
        out_specs=(placed, placed),
        check_vma=False,
    )
```
